32 devices in a mesh: groups: 2 (over y), blk: 4 (over z), heads: 2 (over x), beam: 2 (over core).
Axes of the slice: x: 2, y: 2, z: 4, core: 2. Of those that a mesh axis runs over, the one named last changes fastest.
Arguments:
- queries: bfloat16 [4, 32, 64, 128], P(('groups', 'beam'), 'blk', 'heads'), parts along dimension 0, may hold values from -110 to 110
- positions: int32 [4, 32], P(('groups', 'beam'), 'blk'), parts along dimension 0, may hold values from 512 to 4096
- row_order: int32 [4, 32], P(('groups', 'beam')), parts along dimension 0, may hold values from 0 to 31, each once within a row
- lengths: int32 [8], P(('groups', 'blk')), parts along dimension 0, may hold values from 128 to 1024
- cache_keys: bfloat16 [8, 4, 1024, 128], P(('groups', 'blk'), 'heads'), parts along dimension 0, may hold values from -4 to 4
- cache_values: bfloat16 [8, 4, 1024, 128], P(('groups', 'blk'), 'heads'), parts along dimension 0, may hold values from -6 to 6
Outputs:
- attended: bfloat16 [4, 32, 64, 128], P(('groups', 'beam'), 'blk', 'heads'), parts along dimension 0
The draws below stay inside these ranges and needn't reach their ends.
There are 2 independent parts, one for each index of `groups`. The reference program is written for one: setup_inputs(seed, part) draws one part's arguments, and reference() takes and returns one part's arrays. A program takes and returns all parts, laid end to end along the dimension named above; each array names one. Nothing has to cross between parts.
Inputs may be any that keep to these rules, and one draw needn't show every extreme that they name: Slots of shard s from lengths[s] on hold no cache entry. `positions`: a row reads the cache entries whose global position, counted shard after shard as in the reference program, lies below its position. row_order[e] is a permutation of 0 to 31.
All inputs are finite; a program needn't handle non-finite values.
Results may differ from the reference program's by a relative error of at most 0.0015.
Values may be sent and summed in bfloat16 or wider, within the bound.
A program may use at most 64 MiB of HBM per device.

```python
import math
import jax
import jax.numpy as jnp
from jax import lax

HQ = 64
KVH = 4
HD = 128
CAP = 1024
KB = 256
GQ = 16
SETS = 2
SHARDS = 4
ROWS_SET = 32
CONTEXT = 4096


def base_keys(key):
    drawn = jax.random.normal(jax.random.fold_in(key, 11), (SHARDS, KVH, CAP, HD), jnp.float32)
    drawn = jnp.clip(drawn, -4.0, 4.0)
    return drawn


def draw_cache_keys(key, part):
    return base_keys(key).astype(jnp.bfloat16)


def draw_queries(key, part):
    full_shape = (SETS, ROWS_SET, HQ, HD)
    scales = jnp.exp(jax.random.uniform(jax.random.fold_in(key, 26), (SETS, ROWS_SET, HQ, 1), jnp.float32, 0.0, math.log(12.0)))
    entries = jnp.clip(2.5 * scales * jax.random.normal(jax.random.fold_in(key, 25), full_shape, jnp.float32), -110.0, 110.0)
    return entries.astype(jnp.bfloat16)


def plant(values, key, low, largest):
    extent = values.shape
    index_at = [jax.random.randint(jax.random.fold_in(key, axis), (), 0, extent[axis]) for axis in range(len(extent))]
    values = values.at[tuple(index_at)].set(low)
    longest = extent.index(max(extent))
    index_at[longest] = (index_at[longest] + 1) % extent[longest]
    return values.at[tuple(index_at)].set(largest)


def levels(rng, shape, pieces, low, high):
    factor_of = 1.0
    for axis_at, blocks in pieces:
        draws = jax.random.uniform(jax.random.fold_in(jax.random.fold_in(rng, 6), axis_at), (blocks,), jnp.float32, low / len(pieces), high / len(pieces))
        factor_of = factor_of * jnp.repeat(jnp.exp(draws), shape[axis_at] // blocks).reshape((-1,) + (1,) * (len(shape) - 1 - axis_at))
    return factor_of


def bell_draw(rng, dims, width, reach, pieces=(), kind=jnp.bfloat16):
    level = levels(rng, dims, pieces, -0.22, 0.18) if pieces else 1.0
    values = jax.random.normal(rng, dims, jnp.float32) * width * level
    return jnp.minimum(jnp.maximum(values, -reach), reach).astype(kind)


def setup_inputs(seed: int = 0, part: int = 0) -> dict:
    key_list = jax.random.split(jax.random.key(seed), 7)
    own_keys = jax.random.split(jax.random.fold_in(key_list[6], part), 7)
    return {
        "queries": draw_queries(jax.random.fold_in(jax.random.fold_in(key_list[6], part), 71), part),
        "positions": plant(jax.random.randint(own_keys[1], (SETS, ROWS_SET), CONTEXT // 8, CONTEXT + 1), jax.random.fold_in(own_keys[1], 1), CONTEXT // 8, CONTEXT).astype(jnp.int32),
        "row_order": jax.vmap(lambda own: jax.random.permutation(own, ROWS_SET))(jax.random.split(own_keys[2], SETS)).reshape((SETS, ROWS_SET)).astype(jnp.int32),
        "lengths": plant(jax.random.randint(own_keys[3], (SHARDS,), CAP // 8, CAP + 1), jax.random.fold_in(own_keys[3], 1), CAP // 8, CAP).astype(jnp.int32),
        "cache_keys": draw_cache_keys(jax.random.fold_in(jax.random.fold_in(key_list[6], part), 71), part),
        "cache_values": bell_draw(own_keys[5], (SHARDS, KVH, CAP, HD), 1.0, 6.0, ((0, 4), (1, 2))),
    }


masked_score = -1.0e30


def combine_parts(running, latest):
    run_out, run_tot, run_top = running
    new_out, new_tot, new_top = latest
    joined = jnp.maximum(run_top, new_top)
    older = jnp.exp(run_top - joined)
    newer = jnp.exp(new_top - joined)
    return (run_out * older[..., None] + new_out * newer[..., None], run_tot * older + new_tot * newer, joined)


def reference(queries, positions, row_order, lengths, cache_keys, cache_values):
    scaling = float(HD) ** -0.5
    offsets = (jnp.cumsum(lengths) - lengths).astype(jnp.int32)
    query_all = queries.astype(jnp.float32).reshape(SETS, ROWS_SET, KVH, GQ, HD)
    initial = (jnp.zeros((SETS, ROWS_SET, KVH, GQ, HD), jnp.float32),
               jnp.zeros((SETS, ROWS_SET, KVH, GQ), jnp.float32),
               jnp.full((SETS, ROWS_SET, KVH, GQ), masked_score, jnp.float32))

    def per_shard(running, shard_data):
        key_shard, value_shard, offset, length = shard_data
        for block in range(CAP // KB):
            first_slot = block * KB
            key_block = key_shard[:, first_slot:first_slot + KB].astype(jnp.float32)
            value_block = value_shard[:, first_slot:first_slot + KB].astype(jnp.float32)
            scores = jnp.einsum("erkgd,kjd->erkgj", query_all, key_block) * scaling
            slot_ids = first_slot + jnp.arange(KB, dtype=jnp.int32)
            visible = (slot_ids < length)[None, None, :] & ((offset + slot_ids)[None, None, :] < positions[:, :, None])
            visible = visible[:, :, None, None, :]
            highest = jnp.max(jnp.where(visible, scores, masked_score), axis=-1)
            weights = jnp.where(visible, jnp.exp(scores - highest[..., None]), 0.0)
            totals = jnp.sum(weights, axis=-1)
            rounded = lax.optimization_barrier(weights.astype(jnp.bfloat16)).astype(jnp.float32)
            block_out = jnp.einsum("erkgj,kjd->erkgd", rounded, value_block)
            running = combine_parts(running, (block_out, totals, highest))
        return running, None

    final, unused = lax.scan(per_shard, initial, (cache_keys, cache_values, offsets, lengths))
    result = final[0] / final[1][..., None]
    result = result.reshape(SETS, ROWS_SET, HQ, HD)
    placed = jax.vmap(lambda chosen, indices: chosen[indices])(result, row_order.astype(jnp.int32))
    return placed.astype(jnp.bfloat16)
```

```python
import functools
import math

import jax
import jax.numpy as jnp
from jax import lax
from jax.experimental import pallas as pl
from jax.experimental.pallas import tpu as pltpu
from jax.sharding import PartitionSpec as P

KB = 256
MASKED = -1e30
FLOOR = -1e29
MESH = pl.DeviceIdType.MESH


def flipped(place, mask, bits):
    total = 0
    for bit in range(bits):
        digit = lax.rem(lax.div(place, 1 << bit), 2)
        total = total + lax.rem(digit + ((mask >> bit) & 1), 2) * (1 << bit)
    return total


def kernel(
    n, scale,
    pos_ref, order_ref, len_ref, q_hbm, k_hbm, v_hbm,
    out_ref,
    meta, q_all, k_buf, v_buf, vt_buf, sent, came,
    local_sem, relay_send, relay_recv, part_send, part_recv,
):
    me = lax.axis_index("blk")
    rows, kv, group, width = q_hbm.shape
    cap = k_hbm.shape[1]
    lanes = rows * group
    bits = n.bit_length() - 1

    q_in = [
        pltpu.make_async_copy(
            q_hbm.at[:, h], q_all.at[h, pl.ds(me * rows, rows)], local_sem.at[2 * kv + h]
        )
        for h in range(kv)
    ]
    k_in = [pltpu.make_async_copy(k_hbm.at[h], k_buf.at[h], local_sem.at[h]) for h in range(kv)]
    v_in = [pltpu.make_async_copy(v_hbm.at[h], v_buf.at[h], local_sem.at[kv + h]) for h in range(kv)]
    for copy in q_in + k_in + v_in:
        copy.start()

    for r in range(rows):
        meta[me, pl.ds(r, 1), :] = jnp.full((1, 128), pos_ref[0, r], jnp.int32)
    meta[me, pl.ds(rows, 1), :] = jnp.full((1, 128), len_ref[0], jnp.int32)

    barrier = pltpu.get_barrier_semaphore()
    has = {1: me + 1 < n, -1: me >= 1}
    for k in range(1, n):
        pl.semaphore_signal(
            barrier, inc=1, device_id={"blk": flipped(me, k, bits)}, device_id_type=MESH
        )
    pl.semaphore_wait(barrier, n - 1)

    def slot(item, source):
        if item == 0:
            return meta.at[source]
        return q_all.at[item - 1, pl.ds(source * rows, rows)]

    def relay(item, step, hops):
        way = 0 if step == 1 else 1
        block = slot(item, me - step * hops)
        return pltpu.make_async_remote_copy(
            src_ref=block, dst_ref=block,
            send_sem=relay_send.at[item, way, hops],
            recv_sem=relay_recv.at[item, way, hops + 1],
            device_id={"blk": me + step}, device_id_type=MESH,
        )

    def arrival(item, step, hops):
        way = 0 if step == 1 else 1
        block = slot(item, me - step * hops)
        return pltpu.make_async_remote_copy(
            src_ref=block, dst_ref=block,
            send_sem=relay_send.at[item, way, hops],
            recv_sem=relay_recv.at[item, way, hops],
            device_id={"blk": me - step}, device_id_type=MESH,
        )

    def begin(item):
        for step in (1, -1):
            @pl.when(has[step])
            def _():
                relay(item, step, 0).start()

    def turn(item, hops):
        for step in (1, -1):
            source = me - step * hops
            there = (source >= 0) & (source < n)

            @pl.when(there)
            def _():
                arrival(item, step, hops).wait_recv()

            @pl.when(there & has[step])
            def _():
                relay(item, step, hops).start()

    begin(0)
    for h in range(kv):
        q_in[h].wait()
        begin(1 + h)

    for h in range(kv):
        v_in[h].wait()
        vt_buf[h] = v_buf[h].astype(jnp.float32).T.astype(jnp.bfloat16)

    for hops in range(1, n):
        turn(0, hops)
        for h in range(kv):
            turn(1 + h, hops)

    length = meta[me, pl.ds(rows, 1), :]
    offset = jnp.zeros((1, 128), jnp.int32)
    for s in range(n):
        offset = offset + jnp.where(s < me, meta[s, pl.ds(rows, 1), :], 0)
    lane_row = lax.broadcasted_iota(jnp.int32, (1, lanes), 1) // group
    slot_ids = lax.broadcasted_iota(jnp.int32, (KB, lanes), 0)

    def part(h, dest):
        pieces = []
        limit = jnp.zeros((1, lanes), jnp.int32)
        for r in range(rows):
            row = order_ref[0, dest * rows + r]
            pieces.append(q_all[h, row])
            limit = jnp.where(lane_row == r, meta[row // rows, pl.ds(row % rows, 1), :], limit)
        query = jnp.concatenate(pieces, axis=0)
        limit = jnp.minimum(length, limit - offset)
        outs, tots, tops = [], [], []
        for b in range(cap // KB):
            scores = lax.dot_general(
                k_buf[h, pl.ds(b * KB, KB), :], query, (((1,), (1,)), ((), ())),
                preferred_element_type=jnp.float32,
            )
            scores = jnp.where(slot_ids < limit - b * KB, scores, MASKED)
            top = jnp.max(scores, axis=0, keepdims=True)
            weights = jnp.exp2((scores - jnp.maximum(top, FLOOR)) * scale)
            tots.append(jnp.sum(weights, axis=0, keepdims=True))
            tops.append(top)
            outs.append(
                jnp.dot(
                    vt_buf[h, :, pl.ds(b * KB, KB)], weights.astype(jnp.bfloat16),
                    preferred_element_type=jnp.float32,
                )
            )
        return merge(outs, tots, tops)

    def merge(outs, tots, tops):
        best = functools.reduce(jnp.maximum, tops)
        out = tot = 0.0
        for o, t, p in zip(outs, tots, tops):
            factor = jnp.exp2((p - best) * scale)
            out = out + o * factor
            tot = tot + t * factor
        return out, tot, best

    def parcel(h, k):
        return pltpu.make_async_remote_copy(
            src_ref=sent.at[h, k], dst_ref=came.at[h, k],
            send_sem=part_send.at[h, k], recv_sem=part_recv.at[h, k],
            device_id={"blk": flipped(me, k, bits)}, device_id_type=MESH,
        )

    own = []
    for h in range(kv):
        k_in[h].wait()
        for k in range(n - 1, -1, -1):
            out, tot, top = part(h, flipped(me, k, bits))
            if k == 0:
                own.append((out, tot, top))
            else:
                sent[h, k, pl.ds(0, width), :] = out
                sent[h, k, pl.ds(width, 1), :] = tot
                sent[h, k, pl.ds(width + 1, 1), :] = top
                parcel(h, k).start()

    for h in range(kv):
        outs, tots, tops = ([x] for x in own[h])
        for k in range(n - 1, 0, -1):
            parcel(h, k).wait_recv()
            outs.append(came[h, k, pl.ds(0, width), :])
            tots.append(came[h, k, pl.ds(width, 1), :])
            tops.append(came[h, k, pl.ds(width + 1, 1), :])
        out, tot, _ = merge(outs, tots, tops)
        out_ref[:, h] = (out / tot).T.astype(jnp.bfloat16).reshape(rows, group, width)

    for h in range(kv):
        for k in range(n - 1, 0, -1):
            parcel(h, k).wait_send()
    for item in range(1 + kv):
        for hops in range(n - 1):
            for step in (1, -1):
                source = me - step * hops

                @pl.when((source >= 0) & (source < n) & has[step])
                def _():
                    relay(item, step, hops).wait_send()


def per_device(n, queries, positions, row_order, lengths, cache_keys, cache_values):
    keys, values = cache_keys[0], cache_values[0]
    kv, cap, width = keys.shape
    rows = queries.shape[1]
    group = queries.shape[2] // kv
    scale = float(width) ** -0.5 * math.log2(math.e)
    lanes = rows * group
    smem = pl.BlockSpec(memory_space=pltpu.SMEM)
    hbm = pl.BlockSpec(memory_space=pl.ANY)
    out = pl.pallas_call(
        functools.partial(kernel, n, scale),
        out_shape=jax.ShapeDtypeStruct((rows, kv, group, width), jnp.bfloat16),
        in_specs=[smem, smem, smem, hbm, hbm, hbm],
        out_specs=pl.BlockSpec(memory_space=pltpu.VMEM),
        scratch_shapes=[
            pltpu.VMEM((n, 2 * rows, 128), jnp.int32),
            pltpu.VMEM((kv, n * rows, group, width), jnp.bfloat16),
            pltpu.VMEM((kv, cap, width), jnp.bfloat16),
            pltpu.VMEM((kv, cap, width), jnp.bfloat16),
            pltpu.VMEM((kv, width, cap), jnp.bfloat16),
            pltpu.VMEM((kv, n, width + 8, lanes), jnp.float32),
            pltpu.VMEM((kv, n, width + 8, lanes), jnp.float32),
            pltpu.SemaphoreType.DMA((3 * kv,)),
            pltpu.SemaphoreType.DMA((1 + kv, 2, n)),
            pltpu.SemaphoreType.DMA((1 + kv, 2, n)),
            pltpu.SemaphoreType.DMA((kv, n)),
            pltpu.SemaphoreType.DMA((kv, n)),
        ],
        compiler_params=pltpu.CompilerParams(collective_id=0, has_side_effects=True),
        name="attend",
    )(
        positions, row_order, lengths,
        queries.reshape(rows, kv, group, width), keys, values,
    )
    return out.reshape(queries.shape)


def solution(mesh):
    placed = (
        P(("groups", "beam"), "blk", "heads", None),
        P(("groups", "beam"), "blk"),
        P(("groups", "beam"), None),
        P(("groups", "blk")),
        P(("groups", "blk"), "heads", None, None),
        P(("groups", "blk"), "heads", None, None),
    )
    return jax.shard_map(
        functools.partial(per_device, mesh.shape["blk"]),
        mesh=mesh,
        in_specs=placed,
        out_specs=P(("groups", "beam"), "blk", "heads", None),
        check_vma=False,
    )
```

```python
import functools
import math

import jax
import jax.numpy as jnp
from jax import lax
from jax.experimental import pallas as pl
from jax.experimental.pallas import tpu as pltpu
from jax.sharding import PartitionSpec as P

KB = 256
MASKED = -1e30
FLOOR = -1e29
MESH = pl.DeviceIdType.MESH


def flipped(place, mask, bits):
    total = 0
    for bit in range(bits):
        digit = lax.rem(lax.div(place, 1 << bit), 2)
        total = total + lax.rem(digit + ((mask >> bit) & 1), 2) * (1 << bit)
    return total


def kernel(
    n, scale,
    pos_ref, order_ref, len_ref, q_hbm, k_hbm, v_hbm,
    out_ref,
    meta, q_all, k_buf, v_buf, vt_buf, sent, came,
    local_sem, relay_send, relay_recv, part_send, part_recv,
):
    me = lax.axis_index("blk")
    rows, kv, group, width = q_hbm.shape
    cap = k_hbm.shape[1]
    lanes = rows * group
    bits = n.bit_length() - 1

    q_in = [
        pltpu.make_async_copy(
            q_hbm.at[:, h], q_all[h].at[pl.ds(me * rows, rows)], local_sem.at[2 * kv + h]
        )
        for h in range(kv)
    ]
    k_in = [pltpu.make_async_copy(k_hbm.at[h], k_buf.at[h], local_sem.at[h]) for h in range(kv)]
    v_in = [pltpu.make_async_copy(v_hbm.at[h], v_buf.at[h], local_sem.at[kv + h]) for h in range(kv)]
    for copy in q_in + k_in + v_in:
        copy.start()

    for r in range(rows):
        meta[me, pl.ds(r, 1), :] = jnp.full((1, 128), pos_ref[0, r], jnp.int32)
    meta[me, pl.ds(rows, 1), :] = jnp.full((1, 128), len_ref[0], jnp.int32)

    barrier = pltpu.get_barrier_semaphore()
    has = {1: me + 1 < n, -1: me >= 1}
    for step in (1, -1):
        @pl.when(has[step])
        def _():
            pl.semaphore_signal(barrier, inc=1, device_id={"blk": me + step}, device_id_type=MESH)

    pl.semaphore_wait(barrier, has[1].astype(jnp.int32) + has[-1].astype(jnp.int32))

    def slot(item, source):
        if item == 0:
            return meta.at[source]
        return q_all[item - 1].at[pl.ds(source * rows, rows)]

    def relay(item, step, hops):
        way = 0 if step == 1 else 1
        block = slot(item, me - step * hops)
        return pltpu.make_async_remote_copy(
            src_ref=block, dst_ref=block,
            send_sem=relay_send.at[item, way, hops],
            recv_sem=relay_recv.at[item, way, hops + 1],
            device_id={"blk": me + step}, device_id_type=MESH,
        )

    def arrival(item, step, hops):
        way = 0 if step == 1 else 1
        block = slot(item, me - step * hops)
        return pltpu.make_async_remote_copy(
            src_ref=block, dst_ref=block,
            send_sem=relay_send.at[item, way, hops],
            recv_sem=relay_recv.at[item, way, hops],
            device_id={"blk": me - step}, device_id_type=MESH,
        )

    def begin(item):
        for step in (1, -1):
            @pl.when(has[step])
            def _():
                relay(item, step, 0).start()

    def turn(item, hops):
        for step in (1, -1):
            source = me - step * hops
            there = (source >= 0) & (source < n)

            @pl.when(there)
            def _():
                arrival(item, step, hops).wait_recv()

            @pl.when(there & has[step])
            def _():
                relay(item, step, hops).start()

    begin(0)
    for h in range(kv):
        q_in[h].wait()
        begin(1 + h)

    for h in range(kv):
        v_in[h].wait()
        vt_buf[h] = v_buf[h].astype(jnp.float32).T.astype(jnp.bfloat16)

    for hops in range(1, n):
        turn(0, hops)
        turn(1, hops)
        if hops == 1:
            for h in range(1, kv):
                turn(1 + h, hops)

    length = meta[me, pl.ds(rows, 1), :]
    offset = jnp.zeros((1, 128), jnp.int32)
    for s in range(n):
        offset = offset + jnp.where(s < me, meta[s, pl.ds(rows, 1), :], 0)
    lane_row = lax.broadcasted_iota(jnp.int32, (1, lanes), 1) // group
    slot_ids = lax.broadcasted_iota(jnp.int32, (KB, lanes), 0)

    def part(h, dest):
        pieces = []
        limit = jnp.zeros((1, lanes), jnp.int32)
        for r in range(rows):
            row = order_ref[0, dest * rows + r]
            pieces.append(q_all[h][row])
            limit = jnp.where(lane_row == r, meta[row // rows, pl.ds(row % rows, 1), :], limit)
        query = jnp.concatenate(pieces, axis=0)
        limit = jnp.minimum(length, limit - offset)
        outs, tots, tops = [], [], []
        for b in range(cap // KB):
            scores = lax.dot_general(
                k_buf[h, pl.ds(b * KB, KB), :], query, (((1,), (1,)), ((), ())),
                preferred_element_type=jnp.float32,
            )
            scores = jnp.where(slot_ids < limit - b * KB, scores, MASKED)
            top = jnp.max(scores, axis=0, keepdims=True)
            weights = jnp.exp2((scores - jnp.maximum(top, FLOOR)) * scale)
            tots.append(jnp.sum(weights, axis=0, keepdims=True))
            tops.append(top)
            outs.append(
                jnp.dot(
                    vt_buf[h, :, pl.ds(b * KB, KB)], weights.astype(jnp.bfloat16),
                    preferred_element_type=jnp.float32,
                )
            )
        return merge(outs, tots, tops)

    def merge(outs, tots, tops):
        best = functools.reduce(jnp.maximum, tops)
        out = tot = 0.0
        for o, t, p in zip(outs, tots, tops):
            factor = jnp.exp2((p - best) * scale)
            out = out + o * factor
            tot = tot + t * factor
        return out, tot, best

    def parcel(h, k):
        return pltpu.make_async_remote_copy(
            src_ref=sent.at[h, k], dst_ref=came.at[h, k],
            send_sem=part_send.at[h, k], recv_sem=part_recv.at[h, k],
            device_id={"blk": flipped(me, k, bits)}, device_id_type=MESH,
        )

    own = []
    for h in range(kv):
        k_in[h].wait()
        for k in range(n - 1, -1, -1):
            out, tot, top = part(h, flipped(me, k, bits))
            if k == 0:
                own.append((out, tot, top))
            else:
                sent[h, k, pl.ds(0, width), :] = out
                sent[h, k, pl.ds(width, 1), :] = tot
                sent[h, k, pl.ds(width + 1, 1), :] = top
                parcel(h, k).start()
            if h + 1 < kv and 2 <= n - k + 1 < n:
                turn(2 + h, n - k + 1)

    for h in range(kv):
        outs, tots, tops = ([x] for x in own[h])
        for k in range(n - 1, 0, -1):
            parcel(h, k).wait_recv()
            outs.append(came[h, k, pl.ds(0, width), :])
            tots.append(came[h, k, pl.ds(width, 1), :])
            tops.append(came[h, k, pl.ds(width + 1, 1), :])
        out, tot, _ = merge(outs, tots, tops)
        out_ref[:, h] = (out / tot).T.astype(jnp.bfloat16).reshape(rows, group, width)

    for h in range(kv):
        for k in range(n - 1, 0, -1):
            parcel(h, k).wait_send()
    for item in range(1 + kv):
        for hops in range(n - 1):
            for step in (1, -1):
                source = me - step * hops

                @pl.when((source >= 0) & (source < n) & has[step])
                def _():
                    relay(item, step, hops).wait_send()


def per_device(n, queries, positions, row_order, lengths, cache_keys, cache_values):
    keys, values = cache_keys[0], cache_values[0]
    kv, cap, width = keys.shape
    rows = queries.shape[1]
    group = queries.shape[2] // kv
    scale = float(width) ** -0.5 * math.log2(math.e)
    lanes = rows * group
    smem = pl.BlockSpec(memory_space=pltpu.SMEM)
    hbm = pl.BlockSpec(memory_space=pl.ANY)
    out = pl.pallas_call(
        functools.partial(kernel, n, scale),
        out_shape=jax.ShapeDtypeStruct((rows, kv, group, width), jnp.bfloat16),
        in_specs=[smem, smem, smem, hbm, hbm, hbm],
        out_specs=pl.BlockSpec(memory_space=pltpu.VMEM),
        scratch_shapes=[
            pltpu.VMEM((n, 2 * rows, 128), jnp.int32),
            [pltpu.VMEM((n * rows, group, width), jnp.bfloat16) for _ in range(kv)],
            pltpu.VMEM((kv, cap, width), jnp.bfloat16),
            pltpu.VMEM((kv, cap, width), jnp.bfloat16),
            pltpu.VMEM((kv, width, cap), jnp.bfloat16),
            pltpu.VMEM((kv, n, width + 8, lanes), jnp.float32),
            pltpu.VMEM((kv, n, width + 8, lanes), jnp.float32),
            pltpu.SemaphoreType.DMA((3 * kv,)),
            pltpu.SemaphoreType.DMA((1 + kv, 2, n)),
            pltpu.SemaphoreType.DMA((1 + kv, 2, n)),
            pltpu.SemaphoreType.DMA((kv, n)),
            pltpu.SemaphoreType.DMA((kv, n)),
        ],
        compiler_params=pltpu.CompilerParams(collective_id=0, has_side_effects=True),
        name="attend",
    )(
        positions, row_order, lengths,
        queries.reshape(rows, kv, group, width), keys, values,
    )
    return out.reshape(queries.shape)


def solution(mesh):
    placed = (
        P(("groups", "beam"), "blk", "heads", None),
        P(("groups", "beam"), "blk"),
        P(("groups", "beam"), None),
        P(("groups", "blk")),
        P(("groups", "blk"), "heads", None, None),
        P(("groups", "blk"), "heads", None, None),
    )
    return jax.shard_map(
        functools.partial(per_device, mesh.shape["blk"]),
        mesh=mesh,
        in_specs=placed,
        out_specs=P(("groups", "beam"), "blk", "heads", None),
        check_vma=False,
    )
```
